256 devices in a mesh: groups: 2 (over z), seq: 16 (over y, core), head: 8 (over x).
Axes of the slice: x: 8, y: 8, z: 2, core: 2. Of those that a mesh axis runs over, the one named last changes fastest.
The devices are a block of a 8x8x16 slice.
Arguments:
- queries: bfloat16 [4096, 8192], P(('groups', 'seq'), 'head'), parts along dimension 0
- new_keys: bfloat16 [4096, 1024], P(('groups', 'seq'), 'head'), parts along dimension 0, may hold values from -6 to 6
- new_values: bfloat16 [4096, 1024], P(('groups', 'seq'), 'head'), parts along dimension 0, may hold values from -6 to 6
- cache_keys: bfloat16 [32768, 1024], P(('groups', 'seq'), 'head'), parts along dimension 0
- cache_values: bfloat16 [32768, 1024], P(('groups', 'seq'), 'head'), parts along dimension 0, may hold values from -6 to 6
- valid_len: int32 [32], P('groups'), parts along dimension 0, may hold values from 1 to 1024, as said below
- block_of: int32 [32], P('groups'), parts along dimension 0, may hold values from 0 to 15, each once
Outputs:
- attended: bfloat16 [4096, 8192], P(('groups', 'seq'), 'head'), parts along dimension 0
The draws below stay inside these ranges and needn't reach their ends.
There are 2 independent parts, one for each index of `groups`. The reference program is written for one: setup_inputs(seed, part) draws one part's arguments, and reference() takes and returns one part's arrays. A program takes and returns all parts, laid end to end along the dimension named above; each array names one. Nothing has to cross between parts.
Inputs may be any that keep to these rules, and one draw needn't show every extreme that they name: `valid_len`: some shard is full (1024 filled slots) in every draw; slot 0 of every shard is filled. `block_of`: A permutation of the 16 span blocks.
All inputs are finite; a program needn't handle non-finite values.
Results may differ from the reference program's by a relative error of at most 0.0027.
Values may be sent and summed in bfloat16 or wider, within the bound.
No kernel may reach another device: no remote copies, remote signals or barrier semaphores. Data moves between devices by JAX's collectives and lax.ppermute only.
A program may use at most 192 MiB of HBM per device.

```python
import math
import jax
import jax.numpy as jnp
from jax import lax

HQ = 64
KV = 8
DH = 128
GROUP = 8
CB = 128
LEN_DEV = 1024
SPAN = 2048
CONTEXT = 16384
N_SEQ = 16


def draw_queries(key, part):
    shape = (SPAN, HQ * DH)
    drawn = jnp.clip(jax.random.normal(key, shape, jnp.float32), -6.0, 6.0)
    return drawn.astype(jnp.bfloat16)


def draw_cache_keys(key, part):
    shape = (CONTEXT, KV * DH)
    drawn = jnp.clip(jax.random.normal(key, shape, jnp.float32), -6.0, 6.0)
    return drawn.astype(jnp.bfloat16)


def draw_valid_len(key, part):
    filled = jax.random.randint(jax.random.fold_in(key, 3), (N_SEQ,), 1, LEN_DEV + 1)
    full_one = jax.random.randint(jax.random.fold_in(key, 5), (), 0, N_SEQ)
    return filled.at[full_one].set(LEN_DEV).astype(jnp.int32)


def shard_levels(rng, shape, cuts, smallest, largest):
    factor_of, own = 1.0, jax.random.fold_in(rng, 6)
    for axis_at, parts in cuts:
        heights = jnp.exp(jax.random.uniform(jax.random.fold_in(own, axis_at), (parts,), jnp.float32, smallest / len(cuts), largest / len(cuts)))
        factor_of = factor_of * jnp.repeat(heights, shape[axis_at] // parts).reshape([-1 if axis == axis_at else 1 for axis in range(len(shape))])
    return factor_of


def bell_draw(key, dims, scale, limit, pieces=(), kind=jnp.bfloat16):
    values = scale * jax.random.normal(key, dims, jnp.float32)
    if pieces:
        values = values * shard_levels(key, dims, pieces, -0.22, 0.18)
    return jnp.clip(values, -limit, limit).astype(kind)


def setup_inputs(seed: int = 0, part: int = 0) -> dict:
    streams_of = jax.random.split(jax.random.key(seed), 8)
    part_splits = jax.random.split(jax.random.fold_in(streams_of[7], part), 8)
    queries = draw_queries(jax.random.fold_in(jax.random.fold_in(streams_of[7], part), 71), part)
    new_keys = bell_draw(part_splits[1], (SPAN, KV * DH), 1.0, 6.0, ((0, 16), (1, 8)))
    new_values = bell_draw(part_splits[2], (SPAN, KV * DH), 1.0, 6.0, ((0, 16), (1, 8)))
    cache_keys = draw_cache_keys(jax.random.fold_in(jax.random.fold_in(streams_of[7], part), 71), part)
    cache_values = bell_draw(part_splits[4], (CONTEXT, KV * DH), 1.0, 6.0, ((0, 16), (1, 8)))
    valid_len = draw_valid_len(jax.random.fold_in(jax.random.fold_in(streams_of[7], part), 71), part)
    block_of = jax.random.permutation(part_splits[6], N_SEQ).astype(jnp.int32)
    return dict(queries=queries, new_keys=new_keys, new_values=new_values, cache_keys=cache_keys, cache_values=cache_values, valid_len=valid_len, block_of=block_of)


def reference(queries, new_keys, new_values, cache_keys, cache_values, valid_len, block_of):
    span = CB * N_SEQ
    context = LEN_DEV * N_SEQ
    rows = jnp.arange(span, dtype=jnp.int32)
    query_pos = block_of[rows // CB].astype(jnp.int32) * CB + rows % CB
    places = jnp.arange(context, dtype=jnp.int32)
    cache_live = (places % LEN_DEV) < valid_len[places // LEN_DEV]
    key_pos = jnp.concatenate([jnp.full((context,), -1, jnp.int32), query_pos])
    key_live = jnp.concatenate([cache_live, jnp.ones((span,), bool)])
    keys_all = jnp.concatenate([cache_keys, new_keys], 0).astype(jnp.float32).reshape(-1, KV, DH)
    values_cache = cache_values.astype(jnp.float32).reshape(N_SEQ, LEN_DEV, KV, DH)
    values_span = new_values.astype(jnp.float32).reshape(N_SEQ, CB, KV, DH)
    width = math.gcd(span, 16)
    count = span // width
    query_blocks = queries.astype(jnp.float32).reshape(count, width, KV, GROUP, DH)
    pos_blocks = query_pos.reshape(count, width)

    def one_block(item):
        block, pos = item
        scores = jnp.einsum("rkgd,nkd->rkgn", block, keys_all) * (DH ** -0.5)
        seen = (key_live[None, :] & (key_pos[None, :] <= pos[:, None]))[:, None, None, :]
        masked = jnp.where(seen, scores, -1.0e30)
        lead = masked.shape[:3]
        cache_part = masked[..., :context].reshape(lead + (N_SEQ, LEN_DEV))
        span_part = masked[..., context:].reshape(lead + (N_SEQ, CB))
        local = jnp.maximum(jnp.max(cache_part, axis=-1), jnp.max(span_part, axis=-1))
        local_full = jnp.concatenate([jnp.repeat(local, LEN_DEV, axis=-1), jnp.repeat(local, CB, axis=-1)], -1)
        weights = jnp.where(seen, jnp.exp(scores - local_full), 0.0)
        rounded = lax.optimization_barrier(weights.astype(jnp.bfloat16)).astype(jnp.float32)
        weights_cache = weights[..., :context].reshape(lead + (N_SEQ, LEN_DEV))
        weights_span = weights[..., context:].reshape(lead + (N_SEQ, CB))
        part_total = jnp.sum(weights_cache, axis=-1) + jnp.sum(weights_span, axis=-1)
        rounded_cache = rounded[..., :context].reshape(lead + (N_SEQ, LEN_DEV))
        rounded_span = rounded[..., context:].reshape(lead + (N_SEQ, CB))
        part_numer = jnp.einsum("rkgsl,slkd->rkgsd", rounded_cache, values_cache)
        part_numer = part_numer + jnp.einsum("rkgsc,sckd->rkgsd", rounded_span, values_span)
        top = jnp.max(local, axis=-1)
        factor = jnp.exp(local - top[..., None])
        numer = jnp.sum(part_numer * factor[..., None], axis=-2)
        total = jnp.sum(part_total * factor, axis=-1)
        return (numer / total[..., None]).astype(jnp.bfloat16).reshape(width, -1)

    result = lax.map(one_block, (query_blocks, pos_blocks))
    return result.reshape(span, HQ * DH)
```

```python
import functools
import math

import jax
import jax.numpy as jnp
from jax import lax
from jax.experimental import pallas as pl
from jax.experimental.pallas import tpu as pltpu
from jax.sharding import PartitionSpec as P

DH = 128
TILE = 256
LANES = 128
NEGATIVE = -1e30
FACTOR = DH**-0.5 * math.log2(math.e)


def attend_kernel(
    step, first, last, row_from, row_to,
    me_ref, valid_ref, block_ref, q_ref, k_ref, v_ref, *refs
):
    if first:
        acc_in = top_in = sum_in = None
    else:
        acc_in, top_in, sum_in = refs[:3]
        refs = refs[3:]
    acc_out, top_out, sum_out, s_ref, m_ref = refs
    size = valid_ref.shape[0]
    me = me_ref[0]
    source = lax.rem(me + step + size, size)
    partner = me + 1 - 2 * lax.rem(me, 2)
    valid = valid_ref[source]
    key_block = block_ref[source]
    rows_all = q_ref.shape[0]
    half = rows_all // 2
    keys_all = k_ref.shape[0]
    span = LANES
    count = lax.div(valid + span + TILE - 1, TILE)
    lane = lax.broadcasted_iota(jnp.int32, (TILE, LANES), 1)
    row = lax.rem(lax.broadcasted_iota(jnp.int32, (TILE, LANES), 0), span)
    ahead = lane - row

    def widths(n):
        return [min(TILE, keys_all - t * TILE) for t in range(n)]

    def scores(n, tile, slot):
        start = pl.multiple_of(tile * TILE, TILE)
        rows = pl.ds(start, TILE)
        query_block = jnp.where(start < half, block_ref[me], block_ref[partner])
        shift = (query_block - key_block) * span
        q = q_ref[rows, :]
        best = None
        for t, width in enumerate(widths(n)):
            s = lax.dot_general(
                q, k_ref[t * TILE : t * TILE + width, :],
                (((1,), (1,)), ((), ())), preferred_element_type=jnp.float32,
            )
            for c in range(width // LANES):
                piece = s[:, c * LANES : (c + 1) * LANES]
                at = t * TILE + c * LANES
                if at == 0:
                    piece = jnp.where(ahead <= shift, piece, NEGATIVE)
                elif t == n - 1:
                    piece = jnp.where(lane < valid + (span - at), piece, NEGATIVE)
                s_ref[slot, :, at : at + LANES] = piece
                best = piece if best is None else jnp.maximum(best, piece)
        m_ref[slot] = best

    def weigh(n, tile, slot):
        rows = pl.ds(pl.multiple_of(tile * TILE, TILE), TILE)
        out_rows = pl.ds(pl.multiple_of(tile * TILE - row_from, TILE), TILE)
        local = jnp.max(m_ref[slot], axis=1, keepdims=True)
        total = None
        numer = None
        for t, width in enumerate(widths(n)):
            pieces = []
            for c in range(width // LANES):
                at = t * TILE + c * LANES
                p = jnp.exp2((s_ref[slot, :, at : at + LANES] - local) * FACTOR)
                total = p if total is None else total + p
                pieces.append(p.astype(jnp.bfloat16))
            weights = pieces[0] if len(pieces) == 1 else jnp.concatenate(pieces, axis=1)
            part = jnp.dot(
                weights, v_ref[t * TILE : t * TILE + width, :],
                preferred_element_type=jnp.float32,
            )
            numer = part if numer is None else numer + part
        local = jnp.broadcast_to(local, (TILE, LANES))
        if first:
            acc_out[out_rows, :] = numer
            top_out[out_rows, :] = local
            sum_out[out_rows, :] = total
            return
        best = top_in[rows, :]
        newest = jnp.maximum(best, local)
        keep = jnp.exp2((best - newest) * FACTOR)
        fresh = jnp.exp2((local - newest) * FACTOR)
        numer = acc_in[rows, :] * keep + numer * fresh
        total = sum_in[rows, :] * keep + total * fresh
        acc_out[out_rows, :] = numer
        top_out[out_rows, :] = newest
        if last:
            total = jnp.broadcast_to(jnp.sum(total, axis=1, keepdims=True), (TILE, LANES))
        sum_out[out_rows, :] = total

    begin, end = row_from // TILE, row_to // TILE
    most = -(-keys_all // TILE)
    for n in range(1, most + 1):

        @pl.when(count == n)
        def _(n=n):
            scores(n, begin, 0)

            def pair(j, carry):
                tile = begin + 2 * j
                scores(n, tile + 1, 1)
                weigh(n, tile, 0)
                scores(n, jnp.minimum(tile + 2, end - 1), 0)
                weigh(n, tile + 1, 1)
                return carry

            lax.fori_loop(0, (end - begin) // 2, pair, 0)


def attend(step, scalars, q, k, v, state, rows=None, last=False):
    row_from, row_to = rows or (0, q.shape[0])
    out = jax.ShapeDtypeStruct((row_to - row_from, LANES), jnp.float32)
    smem = pl.BlockSpec(memory_space=pltpu.SMEM)
    vmem = pl.BlockSpec(memory_space=pltpu.VMEM)
    first = state is None
    states = () if first else tuple(state)
    aliased = {6: 0, 7: 1, 8: 2} if states and rows is None else {}
    keys = k.shape[0]
    return pl.pallas_call(
        functools.partial(attend_kernel, step, first, last, row_from, row_to),
        out_shape=(out,) * 3,
        in_specs=[smem] * 3 + [vmem] * (3 + len(states)),
        out_specs=(vmem,) * 3,
        scratch_shapes=[
            pltpu.VMEM((2, TILE, keys), jnp.float32),
            pltpu.VMEM((2, TILE, LANES), jnp.float32),
        ],
        input_output_aliases=aliased,
        cost_estimate=pl.CostEstimate(
            flops=4 * (row_to - row_from) * keys * LANES,
            bytes_accessed=4 * keys * LANES,
            transcendentals=(row_to - row_from) * keys,
        ),
        compiler_params=pltpu.CompilerParams(vmem_limit_bytes=24 << 20),
        name=f"attend_{step}_{row_from}".replace("-", "m"),
    )(*scalars, q, k, v, *states)


def merge_kernel(acc_a, top_a, sum_a, acc_b, top_b, sum_b, out_ref):
    rows = out_ref.shape[0]
    for h in range(out_ref.shape[1] // DH):
        at = slice(h * rows, (h + 1) * rows)
        best = jnp.maximum(top_a[at, :], top_b[at, :])
        one = jnp.exp2((top_a[at, :] - best) * FACTOR)
        two = jnp.exp2((top_b[at, :] - best) * FACTOR)
        numer = acc_a[at, :] * one + acc_b[at, :] * two
        total = sum_a[at, :] * one + sum_b[at, :] * two
        out_ref[:, h * DH : (h + 1) * DH] = (numer / total).astype(out_ref.dtype)


def merge(mine, theirs, rows, width):
    vmem = pl.BlockSpec(memory_space=pltpu.VMEM)
    return pl.pallas_call(
        merge_kernel,
        out_shape=jax.ShapeDtypeStruct((rows, width), jnp.bfloat16),
        in_specs=[vmem] * 6,
        out_specs=vmem,
        compiler_params=pltpu.CompilerParams(vmem_limit_bytes=16 << 20),
        name="merge",
    )(*mine, *theirs)


def on_device(queries, new_keys, new_values, cache_keys, cache_values, valid_len, block_of):
    size = lax.axis_size("seq")
    rows, width = queries.shape
    heads = width // DH
    right = [(i, (i + 2) % size) for i in range(size)]
    left = [(i, (i - 2) % size) for i in range(size)]
    swap = [(i, i ^ 1) for i in range(size)]

    def go(a, pairs):
        return lax.ppermute(a, "seq", pairs)

    k0 = jnp.concatenate([new_keys, cache_keys], 0)
    v0 = jnp.concatenate([new_values, cache_values], 0)
    mine = queries.reshape(rows, heads, DH).transpose(1, 0, 2).reshape(heads * rows, DH)
    q = jnp.concatenate([mine, go(mine, swap)], 0)
    scalars = (jnp.reshape(lax.axis_index("seq"), (1,)), valid_len, block_of)

    hops = size // 4
    state = attend(0, scalars, q, k0, v0, None)
    kr = kl = k0
    vr = vl = v0
    for hop in range(1, hops):
        kr, kl = go(kr, right), go(kl, left)
        vr, vl = go(vr, right), go(vl, left)
        state = attend(-2 * hop, scalars, q, kr, vr, state)
        state = attend(2 * hop, scalars, q, kl, vl, state)
    k, v = go(kr, right), go(vl, left)
    half = heads * rows
    theirs = attend(2 * hops, scalars, q, k, v, state, (half, 2 * half), True)
    theirs = [go(a, swap) for a in theirs]
    ours = attend(2 * hops, scalars, q, k, v, state, (0, half), True)
    return merge(ours, theirs, rows, width)


def solution(mesh):
    rows = P(("groups", "seq"), "head")
    return jax.shard_map(
        on_device,
        mesh=mesh,
        in_specs=(rows,) * 5 + (P("groups"), P("groups")),
        out_specs=rows,
        check_vma=False,
    )
```

```python
import functools
import math

import jax
import jax.numpy as jnp
from jax import lax
from jax.experimental import pallas as pl
from jax.experimental.pallas import tpu as pltpu
from jax.sharding import PartitionSpec as P


DH = 128
TILE = 256
LANES = 128
ROWS = 512
NEGATIVE = -1e30
FACTOR = DH**-0.5 * math.log2(math.e)


def attend_kernel(
    steps, first, last, row_from, row_to, counts,
    me_ref, valid_ref, block_ref, q_ref, *refs
):
    blocks = len(steps)
    kv_refs, refs = refs[:blocks], refs[blocks:]
    states, refs = ((), refs) if first else (refs[:3], refs[3:])
    many = 1 if last else 3
    outs, (s_ref, m_ref), copies = refs[:many], refs[many : many + 2], refs[many + 2 :]
    whole = row_from == 0 and row_to == q_ref.shape[0]
    acc_in, top_in, sum_in = outs if whole or first else states
    (kv_ref,) = copies or kv_refs
    size = valid_ref.shape[0]
    me = me_ref[0]
    way = 1 - 2 * lax.rem(me, 2)
    partner = me + way
    half = q_ref.shape[0] // 2
    keys_all = kv_ref.shape[0]
    span = LANES
    lane = lax.broadcasted_iota(jnp.int32, (ROWS, LANES), 1)
    row = lax.rem(lax.broadcasted_iota(jnp.int32, (ROWS, LANES), 0), span)
    ahead = lane - row
    begin, end = row_from // ROWS, row_to // ROWS
    unmasked = {n: low * TILE for low, n in zip((0, *counts), counts)}

    def one_block(b, carry):
        here = [lax.rem((me, partner)[of] - 2 * hop * way + size, size) for hop, of in steps]
        source = here[0] if blocks == 1 else jnp.where(b == 0, here[0], here[1])
        valid = valid_ref[source]
        key_block = block_ref[source]
        count = lax.div(valid + span + TILE - 1, TILE)
        for i in range(blocks if copies else 0):

            @pl.when(b == i)
            def _(i=i):
                kv_ref[...] = kv_refs[i][...]

        def scores(n, tile):
            start = pl.multiple_of(tile * ROWS, ROWS)
            query_block = jnp.where(start < half, block_ref[me], block_ref[partner])
            shift = (query_block - key_block) * span
            q = q_ref[pl.ds(start, ROWS), :]
            best = None
            for t in range(n):
                width = min(TILE, keys_all - t * TILE)
                s = lax.dot_general(
                    q, kv_ref[t * TILE : t * TILE + width, :LANES],
                    (((1,), (1,)), ((), ())), preferred_element_type=jnp.float32,
                )
                for c in range(width // LANES):
                    piece = s[:, c * LANES : (c + 1) * LANES]
                    at = t * TILE + c * LANES
                    if at == 0:
                        piece = jnp.where(ahead <= shift, piece, NEGATIVE)
                    elif at + LANES > unmasked[n]:
                        piece = jnp.where(lane < valid + (span - at), piece, NEGATIVE)
                    s_ref[at // LANES] = piece
                    best = piece if best is None else jnp.maximum(best, piece)
            finish(best)

        def finish(best):
            local = jnp.max(best, axis=1, keepdims=True)
            m_ref[...] = jnp.broadcast_to(local, (ROWS, LANES))

        def first_scores():
            shift = (block_ref[me if row_from < half else partner] - key_block) * span
            q = q_ref[row_from : row_from + ROWS, :]
            m_ref[...] = jnp.full((ROWS, LANES), NEGATIVE, jnp.float32)

            def key_tile(t, carry):
                start = pl.multiple_of(jnp.minimum(t * TILE, keys_all - TILE), LANES)
                s = lax.dot_general(
                    q, kv_ref[pl.ds(start, TILE), :LANES],
                    (((1,), (1,)), ((), ())), preferred_element_type=jnp.float32,
                )
                best = m_ref[...]
                for c in range(TILE // LANES):
                    piece = s[:, c * LANES : (c + 1) * LANES]
                    limit = valid + (span - 1) - start - c * LANES
                    if c == 0:
                        seen = lane - jnp.where(t == 0, row, 0) <= jnp.where(t == 0, shift, limit)
                    else:
                        seen = lane <= limit
                    piece = jnp.where(seen, piece, NEGATIVE)
                    s_ref[lax.div(start, LANES) + c] = piece
                    best = jnp.maximum(best, piece)
                m_ref[...] = best
                return carry

            tiles = counts[-1]
            for n in counts[-2::-1]:
                tiles = jnp.where(count <= n, n, tiles)
            lax.fori_loop(0, tiles, key_tile, 0)
            finish(m_ref[...])

        def weigh(n, tile):
            rows = pl.ds(pl.multiple_of(tile * ROWS, ROWS), ROWS)
            out_rows = pl.ds(pl.multiple_of(tile * ROWS - row_from, ROWS), ROWS)
            local = m_ref[...]
            total = None
            numer = None
            for t in range(n):
                width = min(TILE, keys_all - t * TILE)
                pieces = []
                for c in range(width // LANES):
                    p = jnp.exp2((s_ref[t * (TILE // LANES) + c] - local) * FACTOR)
                    total = p if total is None else total + p
                    pieces.append(p.astype(jnp.bfloat16))
                weights = pieces[0] if len(pieces) == 1 else jnp.concatenate(pieces, axis=1)
                part = jnp.dot(
                    weights, kv_ref[t * TILE : t * TILE + width, LANES:],
                    preferred_element_type=jnp.float32,
                )
                numer = part if numer is None else numer + part
            if first:
                for ref, value in zip(outs, (numer, local, total)):
                    ref[out_rows, :] = value
                return
            best = top_in[rows, :]
            newest = jnp.maximum(best, local)
            keep = jnp.exp2((best - newest) * FACTOR)
            fresh = jnp.exp2((local - newest) * FACTOR)
            numer = acc_in[rows, :] * keep + numer * fresh
            total = sum_in[rows, :] * keep + total * fresh
            if last:
                (out,) = outs
                total = jnp.broadcast_to(jnp.sum(total, axis=1, keepdims=True), (ROWS, LANES))
                out[out_rows, :LANES] = numer
                out[out_rows, LANES:] = jnp.where(lane < LANES // 2, newest, total)
                return
            for ref, value in zip(outs, (numer, newest, total)):
                ref[out_rows, :] = value

        if end - begin > 2:
            first_scores()
        for low, n in zip((0, *counts), counts):

            @pl.when((count > low) & (count <= n))
            def _(n=n):
                if end - begin == 2:
                    scores(n, begin)
                    weigh(n, begin)
                    scores(n, begin + 1)
                    weigh(n, begin + 1)
                    return

                def body(tile, carry):
                    weigh(n, tile)
                    scores(n, jnp.minimum(tile + 1, end - 1))
                    return carry

                lax.fori_loop(begin, end, body, 0)

        return carry

    if blocks == 1:
        one_block(0, 0)
    else:
        lax.fori_loop(0, blocks, one_block, 0)


def attend(steps, scalars, q, blocks, state, rows=None, last=False):
    row_from, row_to = rows or (0, q.shape[0])
    out = jax.ShapeDtypeStruct((row_to - row_from, LANES * (1 + last)), jnp.float32)
    many = 1 if last else 3
    smem = pl.BlockSpec(memory_space=pltpu.SMEM)
    vmem = pl.BlockSpec(memory_space=pltpu.VMEM)
    first = state is None
    states = () if first else tuple(state)
    at = 4 + len(blocks)
    aliased = {at + i: i for i in range(3)} if states and rows is None else {}
    keys = blocks[0].shape[0]
    most = -(-keys // TILE)
    counts = (3, most) if last else (2, 3, most)
    scratch = [
        pltpu.VMEM((keys // LANES, ROWS, LANES), jnp.float32),
        pltpu.VMEM((ROWS, LANES), jnp.float32),
    ]
    if len(steps) > 1:
        scratch += [pltpu.VMEM((keys, 2 * LANES), jnp.bfloat16)]
    return pl.pallas_call(
        functools.partial(attend_kernel, steps, first, last, row_from, row_to, counts),
        out_shape=(out,) * many,
        in_specs=[smem] * 3 + [vmem] * (1 + len(blocks) + len(states)),
        out_specs=(vmem,) * many,
        scratch_shapes=scratch,
        input_output_aliases=aliased,
        cost_estimate=pl.CostEstimate(
            flops=4 * (row_to - row_from) * keys * LANES * len(steps),
            bytes_accessed=4 * keys * LANES * len(steps),
            transcendentals=(row_to - row_from) * keys * len(steps),
        ),
        compiler_params=pltpu.CompilerParams(vmem_limit_bytes=24 << 20),
        name="attend",
    )(*scalars, q, *blocks, *states)


def merge_kernel(ours_ref, theirs_ref, out_ref):
    rows = out_ref.shape[0]
    low = lax.broadcasted_iota(jnp.int32, (rows, LANES), 1) < LANES // 2

    def parts(ref, at):
        both = ref[at, LANES:]
        turned = pltpu.roll(both, LANES // 2, 1)
        return ref[at, :LANES], jnp.where(low, both, turned), jnp.where(low, turned, both)

    for h in range(out_ref.shape[1] // DH):
        at = slice(h * rows, (h + 1) * rows)
        acc_a, top_a, sum_a = parts(ours_ref, at)
        acc_b, top_b, sum_b = parts(theirs_ref, at)
        best = jnp.maximum(top_a, top_b)
        one = jnp.exp2((top_a - best) * FACTOR)
        two = jnp.exp2((top_b - best) * FACTOR)
        numer = acc_a * one + acc_b * two
        total = sum_a * one + sum_b * two
        out_ref[:, h * DH : (h + 1) * DH] = (numer / total).astype(out_ref.dtype)


def merge(ours, theirs, rows, width):
    vmem = pl.BlockSpec(memory_space=pltpu.VMEM)
    return pl.pallas_call(
        merge_kernel,
        out_shape=jax.ShapeDtypeStruct((rows, width), jnp.bfloat16),
        in_specs=[vmem] * 2,
        out_specs=vmem,
        compiler_params=pltpu.CompilerParams(vmem_limit_bytes=16 << 20),
        name="merge",
    )(ours, theirs)


def whole(queries, new_keys, new_values, cache_keys, cache_values, valid_len, block_of):
    size = lax.axis_size("seq")
    rows, width = queries.shape
    heads = width // DH
    ring = [(i, (i + 2 - 4 * (i % 2)) % size) for i in range(size)]
    swap = [(i, i ^ 1) for i in range(size)]

    def go(a, pairs):
        return lax.ppermute(a, "seq", pairs)

    own = jnp.concatenate(
        [
            jnp.concatenate([new_keys, cache_keys], 0),
            jnp.concatenate([new_values, cache_values], 0),
        ],
        1,
    )
    mine = queries.reshape(rows, heads, DH).transpose(1, 0, 2).reshape(heads * rows, DH)
    q = jnp.concatenate([mine, go(mine, swap)], 0)
    scalars = (jnp.reshape(lax.axis_index("seq"), (1,)), valid_len, block_of)

    hops = size // 4
    a = go(own, ring)
    b = go(go(own, swap), ring)
    state = attend(((0, 0),), scalars, q, (own,), None)
    for hop in range(1, hops):
        state = attend(((hop, 0),), scalars, q, (a,), state)
        state = attend(((hop, 1),), scalars, q, (b,), state)
        a = go(a, ring)
        if hop + 1 < hops:
            b = go(b, ring)
    half = heads * rows
    (theirs,) = attend(((hops, 0),), scalars, q, (a,), state, (half, 2 * half), True)
    theirs = go(theirs, swap)
    (ours,) = attend(((hops, 0),), scalars, q, (a,), state, (0, half), True)
    return merge(ours, theirs, rows, width)


def solution(mesh):
    rows = P(("groups", "seq"), "head")
    return jax.shard_map(
        whole,
        mesh=mesh,
        in_specs=(rows,) * 5 + (P("groups"), P("groups")),
        out_specs=rows,
        check_vma=False,
    )
```
